32 devices in a mesh: pw: 16 (over z, x, core), ka: 2 (over y).
Axes of the slice: x: 2, y: 2, z: 4, core: 2. Of those that a mesh axis runs over, the one named last changes fastest.
Arguments:
- waves: bfloat16 [2, 2, 32768, 256], P('ka', None, 'pw'), may hold values from -0.125 to 0.125
- projectors: bfloat16 [2, 2, 32768, 2304], P('ka', None, 'pw'), may hold values from -0.125 to 0.125
- projector_order: int32 [2304], replicated, may hold values from 0 to 2303, each once
- shift_map: int32 [32768], P('pw'), may hold values from 0 to 32767, as said below
- charges: float32 [128, 18, 18], replicated, may hold values from -0.125 to 0.125
- atom_phase: float32 [128], replicated, may hold values from -3.140625 to 3.140625
Outputs:
- margins: float32 [2, 256, 2, 256], P('ka', 'pw')
The draws below stay inside these ranges and needn't reach their ends.
Inputs may be any that keep to these rules, and one draw needn't show every extreme that they name: `projector_order`: each projector slot once. `shift_map`: a permutation of the plane waves that maps every aligned block of 2048 plane waves onto itself.
All inputs are finite; a program needn't handle non-finite values.
Results may differ from the reference program's by a relative error of at most 0.0003.
Values may be sent and summed in bfloat16 or wider, within the bound.
No kernel may reach another device: no remote copies, remote signals or barrier semaphores. Data moves between devices by JAX's collectives and lax.ppermute only.
A program may use at most 128 MiB of HBM per device.

```python
import jax
import jax.numpy as jnp
from jax import lax

NB = 256
PPA = 18
PW_DEV = 2048
KPTS = 2
NPW = 32768
ATOMS = 128
NPROJ = 2304


def draw_shift_map(key, part):
    blocks = NPW // PW_DEV
    keys = jax.random.split(key, blocks)
    perms = jax.vmap(lambda single: jax.random.permutation(single, PW_DEV))(keys)
    offsets = (jnp.arange(blocks, dtype=jnp.int32) * PW_DEV)[:, None]
    return (perms.astype(jnp.int32) + offsets).reshape(-1).astype(jnp.int32)


def level_of(rng, extent, shards, low, high):
    def one(position, parts):
        steps = jax.random.uniform(jax.random.fold_in(jax.random.fold_in(rng, 6), position), (parts,), jnp.float32, low / len(shards), high / len(shards))
        return jnp.repeat(jnp.exp(steps), extent[position] // parts).reshape((-1,) + (1,) * (len(extent) - position - 1))

    gain = one(*shards[0])
    for cut in shards[1:]:
        gain = gain * one(*cut)
    return gain


def gaussian(key, dims, width, reach, cuts=(), kind=jnp.bfloat16):
    factor_of = level_of(key, dims, cuts, -0.22, 0.18) if cuts else 1.0
    array = jax.random.normal(key, dims, jnp.float32) * width * factor_of
    return jnp.minimum(jnp.maximum(array, -reach), reach).astype(kind)


def setup_inputs(seed: int = 0) -> dict:
    seeds = jax.random.split(jax.random.key(seed), 7)
    waves = gaussian(seeds[0], (KPTS, 2, NPW, NB), (NPW // 16) ** -0.5, 0.125, ((0, 2), (2, 16)))
    projectors = gaussian(seeds[1], (KPTS, 2, NPW, NPROJ), (NPW // 16) ** -0.5, 0.125, ((0, 2), (2, 16)))
    projector_order = jax.random.permutation(seeds[2], NPROJ).astype(jnp.int32)
    shift_map = draw_shift_map(jax.random.fold_in(seeds[6], 71), 0)
    charges = gaussian(seeds[4], (ATOMS, PPA, PPA), NPROJ ** -0.5, 0.125, (), jnp.float32)
    atom_phase = jnp.clip(jax.random.uniform(seeds[5], (ATOMS,), jnp.float32, -3.140625, 3.140625), -3.140625, 3.140625)
    return {"waves": waves, "projectors": projectors, "projector_order": projector_order, "shift_map": shift_map, "charges": charges, "atom_phase": atom_phase}


def contract(left, right, precision=None):
    return lax.dot_general(left, right, (((0,), (0,)), ((), ())), precision=precision, preferred_element_type=jnp.float32)


def complex_cross(left, right, precision=None):
    real = contract(left[0], right[0], precision) + contract(left[1], right[1], precision)
    imag = contract(left[0], right[1], precision) - contract(left[1], right[0], precision)
    return jnp.stack([real, imag], axis=1)


def reference(waves, projectors, projector_order, shift_map, charges, atom_phase):
    inverse = jnp.argsort(projector_order).astype(jnp.int32)
    sym = 0.5 * (charges + jnp.transpose(charges, (0, 2, 1)))

    def project(pair):
        wave, beta = pair
        real = contract(beta[0], wave[0]) + contract(beta[1], wave[1])
        imag = contract(beta[0], wave[1]) - contract(beta[1], wave[0])
        return jnp.stack([real, imag])[:, inverse, :]

    proj = lax.map(project, (waves, projectors))
    last_wave = waves[0][:, shift_map.astype(jnp.int32), :]
    next_wave = jnp.concatenate([waves[1:], last_wave[None]], axis=0)
    repeated = jnp.repeat(atom_phase, PPA)
    cosine = jnp.cos(repeated)[:, None]
    sine = jnp.sin(repeated)[:, None]
    first = proj[0]
    rotated = jnp.stack([first[0] * cosine + first[1] * sine, first[1] * cosine - first[0] * sine])
    next_proj = jnp.concatenate([proj[1:], rotated[None]], axis=0)

    def margin(items):
        wave, nwave, pk, pn = items
        plane = complex_cross(wave, nwave)
        split = pn.reshape(2, ATOMS, PPA, NB)
        weighted = jnp.einsum("apq,raqj->rapj", sym, split, precision=lax.Precision.HIGHEST).reshape(2, NPROJ, NB)
        aug = complex_cross(pk, weighted, lax.Precision.HIGHEST)
        return plane + aug

    return lax.map(margin, (waves, next_wave, proj, next_proj))
```

```python
import jax
import jax.numpy as jnp
from jax import lax
from jax.experimental import pallas as pl
from jax.experimental.pallas import tpu as pltpu
from jax.sharding import PartitionSpec as P

PPA = 18


def from_behind(block, axis, distance):
    devices = range(lax.axis_size(axis))
    route = [((i - distance) % len(devices), i) for i in devices]
    return lax.ppermute(block, axis, route)


def contract(left, right, precision=None, kind=jnp.float32):
    return lax.dot_general(
        left,
        right,
        (((0,), (0,)), ((), ())),
        precision=precision,
        preferred_element_type=kind,
    )


def place_kernel(order_ref, block_ref, out_ref):
    unroll = 16

    def step(i, carry):
        base = i * unroll
        for j in range(unroll):
            out_ref[pl.ds(order_ref[base + j], 1), :] = block_ref[pl.ds(base + j, 1), :]
        return carry

    lax.fori_loop(0, block_ref.shape[0] // unroll, step, 0)


def place_rows(order, block):
    return pl.pallas_call(
        place_kernel,
        out_shape=jax.ShapeDtypeStruct(block.shape, block.dtype),
        in_specs=[
            pl.BlockSpec(memory_space=pltpu.SMEM),
            pl.BlockSpec(memory_space=pltpu.VMEM),
        ],
        out_specs=pl.BlockSpec(memory_space=pltpu.VMEM),
    )(order, block)


def scatter_stage(pieces, axis, low, count):
    size = lax.axis_size(axis)
    digit = (lax.axis_index(axis) // low) % count
    total = lax.dynamic_index_in_dim(pieces, digit, 0, keepdims=False)
    for shift in range(1, count):
        route = []
        for i in range(size):
            d = (i // low) % count
            route.append((i, i + ((d ^ shift) - d) * low))
        sent = lax.dynamic_index_in_dim(pieces, digit ^ shift, 0, keepdims=False)
        total = total + lax.ppermute(sent, axis, route)
    return total


def staged_scatter(block, axis, order):
    size = lax.axis_size(axis)
    rows = block.shape[0] // size
    digits = sorted(order, reverse=True)
    names = list(digits)
    block = block.reshape([count for _, count in digits] + [rows, block.shape[1]])
    for low, count in order:
        at = names.index((low, count))
        block = scatter_stage(jnp.moveaxis(block, at, 0), axis, low, count)
        names.pop(at)
    return block


def local(waves, projectors, projector_order, shift_map, charges, atom_phase):
    wave = waves[0]
    beta = projectors[0]
    pw_dev, bands = wave.shape[1:]
    size = lax.axis_size("pw")
    last_k = lax.axis_index("ka") == lax.axis_size("ka") - 1
    pw_index = lax.axis_index("pw")
    received = from_behind(wave, "ka", -1)
    flat_beta = beta.reshape(2 * pw_dev, beta.shape[2])
    flat_wave = wave.reshape(2 * pw_dev, bands)
    crossed = jnp.concatenate([wave[1], -wave[0]])
    real = place_rows(projector_order, contract(flat_beta, flat_wave))
    if size % 8 == 0:
        outer = size // 4
        imag_stages = [(1, 2), (4, outer), (2, 2)]
        real_stages = [(1, 2), (2, 2), (4, outer)]
    else:
        imag_stages = real_stages = [(1, size)]
    real = staged_scatter(real, "pw", real_stages)
    imag = place_rows(projector_order, contract(flat_beta, crossed))
    imag = staged_scatter(imag, "pw", imag_stages)
    block = jnp.concatenate([real, imag], axis=1)

    spots = lax.iota(jnp.int32, pw_dev)
    local_map = jnp.where(last_k, shift_map - pw_index * pw_dev, spots)
    chosen = (spots[:, None] == local_map[None, :]).astype(jnp.bfloat16)
    joined = jnp.concatenate([received[0], received[1]], axis=1)
    moved = contract(chosen, joined, kind=jnp.bfloat16)
    moved_real, moved_imag = moved[:, :bands], moved[:, bands:]
    plane = contract(wave[0], moved) + contract(
        wave[1], jnp.concatenate([moved_imag, -moved_real], axis=1)
    )

    atom_dev = block.shape[0] // PPA
    own_charges = lax.dynamic_slice_in_dim(charges, pw_index * atom_dev, atom_dev, 0)
    own_sym = 0.5 * (own_charges + jnp.transpose(own_charges, (0, 2, 1)))
    eye = jnp.eye(atom_dev, dtype=jnp.float32)
    spread = (own_sym[:, :, None, :] * eye[:, None, :, None]).reshape(block.shape[0], block.shape[0])
    own_phase = lax.dynamic_slice_in_dim(atom_phase, pw_index * atom_dev, atom_dev)
    own_phase = jnp.where(last_k, jnp.repeat(own_phase, PPA), 0.0)[:, None]
    cosine, sine = jnp.cos(own_phase), jnp.sin(own_phase)

    ahead = from_behind(block, "ka", -1)
    ahead_real, ahead_imag = ahead[:, :bands], ahead[:, bands:]
    turned = jnp.concatenate(
        [ahead_real * cosine + ahead_imag * sine, ahead_imag * cosine - ahead_real * sine], axis=1
    )
    weighted = contract(spread, turned, lax.Precision.HIGHEST)
    crossed_weighted = jnp.concatenate([weighted[:, bands:], -weighted[:, :bands]], axis=1)
    result = (
        plane
        + contract(real, weighted, lax.Precision.HIGHEST)
        + contract(imag, crossed_weighted, lax.Precision.HIGHEST)
    )
    parts = lax.all_to_all(result.reshape(size, bands // size, 2 * bands), "pw", 0, 0)
    summed = jnp.sum(parts, axis=0)
    return summed.reshape(1, bands // size, 2, bands)


def solution(mesh):
    placed = (P("ka", None, "pw", None), P("ka", None, "pw", None), P(), P("pw"), P(), P())
    return jax.shard_map(
        local, mesh=mesh, in_specs=placed, out_specs=P("ka", "pw", None, None), check_vma=False
    )
```

```python
import jax
import jax.numpy as jnp
from jax import lax
from jax.experimental import pallas as pl
from jax.experimental.pallas import tpu as pltpu
from jax.sharding import PartitionSpec as P

PPA = 18


def from_behind(block, axis, distance):
    devices = range(lax.axis_size(axis))
    route = [((i - distance) % len(devices), i) for i in devices]
    return lax.ppermute(block, axis, route)


def contract(left, right, precision=None, kind=jnp.float32):
    return lax.dot_general(
        left,
        right,
        (((0,), (0,)), ((), ())),
        precision=precision,
        preferred_element_type=kind,
    )


def place_kernel(spot_ref, block_ref, out_ref):
    unroll = 16

    def step(i, carry):
        base = pl.multiple_of(i * unroll, unroll)
        rows = [block_ref[pl.ds(base + j, 1), :] for j in range(unroll)]
        for j in range(unroll):
            out_ref[pl.ds(spot_ref[base + j], 1), :] = rows[j]
        return carry

    lax.fori_loop(0, block_ref.shape[0] // unroll, step, 0)


def place_rows(order, block):
    return pl.pallas_call(
        place_kernel,
        out_shape=jax.ShapeDtypeStruct(block.shape, block.dtype),
        in_specs=[
            pl.BlockSpec(memory_space=pltpu.SMEM),
            pl.BlockSpec(memory_space=pltpu.VMEM),
        ],
        out_specs=pl.BlockSpec(memory_space=pltpu.VMEM),
    )(order, block)


def halve(block, names, low):
    at = names.index(low)
    kept = lax.index_in_dim(block, 0, at, keepdims=False)
    sent = lax.index_in_dim(block, 1, at, keepdims=False)
    route = [(i, i ^ low) for i in range(lax.axis_size("pw"))]
    left = [name for name in names if name != low]
    return kept + lax.ppermute(sent, "pw", route), left


def staged(block, names, order):
    for low in order:
        block, names = halve(block, names, low)
    return block


def scatter_result(result, size, pw_index):
    rows = result.shape[0] // size
    if size % 2:
        parts = lax.all_to_all(result.reshape(size, rows, -1), "pw", 0, 0)
        return jnp.sum(parts, axis=0)
    core = pw_index % 2
    split = result.reshape(size // 2, 2, rows, -1)
    kept = lax.dynamic_index_in_dim(split, core, 1, keepdims=False)
    sent = lax.dynamic_index_in_dim(split, 1 - core, 1, keepdims=False)
    joined = kept + lax.ppermute(sent, "pw", [(i, i ^ 1) for i in range(size)])
    groups = [list(range(c, size, 2)) for c in range(2)]
    parts = lax.all_to_all(joined, "pw", 0, 0, axis_index_groups=groups)
    return jnp.sum(parts, axis=0)


def local(waves, projectors, projector_order, shift_map, charges, atom_phase):
    wave = waves[0]
    beta = projectors[0]
    pw_dev, bands = wave.shape[1:]
    size = lax.axis_size("pw")
    last_k = lax.axis_index("ka") == lax.axis_size("ka") - 1
    pw_index = lax.axis_index("pw")
    received = from_behind(wave, "ka", -1)
    flat_beta = beta.reshape(2 * pw_dev, beta.shape[2])
    flat_wave = wave.reshape(2 * pw_dev, bands)
    crossed = lax.optimization_barrier(jnp.concatenate([wave[1], -wave[0]]))
    real = contract(flat_beta, flat_wave)
    rows = beta.shape[2] // size
    if size >= 4 and size & (size - 1) == 0 and rows % 2 == 0:
        names = [1 << bit for bit in range(size.bit_length() - 1)]
        part = (projector_order // rows) ^ pw_index
        place = jnp.zeros_like(part)
        for low in names:
            place = 2 * place + ((part & low) != 0).astype(jnp.int32)
        spot = place * rows + projector_order % rows
        shape = [2] * len(names) + [rows, bands]
        real, left = halve(place_rows(spot, real).reshape(shape), names, 1)
        imag = contract(flat_beta, crossed)
        imag, real = lax.optimization_barrier((imag, real))
        imag, _ = halve(place_rows(spot, imag).reshape(shape), names, 1)
        other = left[1:2] + left[:1] + left[2:]
        real = staged(real, left, other)
        first = lax.slice_in_dim(imag, 0, rows // 2, axis=len(left))
        second = lax.slice_in_dim(imag, rows // 2, rows, axis=len(left))
        imag = jnp.concatenate([staged(first, left, left), staged(second, left, other)])
    else:
        imag = contract(flat_beta, crossed)
        real = lax.psum_scatter(place_rows(projector_order, real), "pw", tiled=True)
        imag = lax.psum_scatter(place_rows(projector_order, imag), "pw", tiled=True)

    spots = lax.iota(jnp.int32, pw_dev)
    local_map = jnp.where(last_k, shift_map - pw_index * pw_dev, spots)
    chosen = (spots[:, None] == local_map[None, :]).astype(jnp.bfloat16)
    joined = jnp.concatenate([received[0], received[1]], axis=1)
    moved = contract(chosen, joined, kind=jnp.bfloat16)
    moved_real, moved_imag = moved[:, :bands], moved[:, bands:]
    plane = contract(wave[0], moved) + contract(
        wave[1], jnp.concatenate([moved_imag, -moved_real], axis=1)
    )

    real, imag, plane = lax.optimization_barrier((real, imag, plane))
    block = jnp.concatenate([real, imag], axis=1)
    atom_dev = block.shape[0] // PPA
    own_charges = lax.dynamic_slice_in_dim(charges, pw_index * atom_dev, atom_dev, 0)
    own_sym = 0.5 * (own_charges + jnp.transpose(own_charges, (0, 2, 1)))
    eye = jnp.eye(atom_dev, dtype=jnp.float32)
    spread = (own_sym[:, :, None, :] * eye[:, None, :, None]).reshape(block.shape[0], block.shape[0])
    own_phase = lax.dynamic_slice_in_dim(atom_phase, pw_index * atom_dev, atom_dev)
    own_phase = jnp.where(last_k, jnp.repeat(own_phase, PPA), 0.0)[:, None]
    cosine, sine = jnp.cos(own_phase), jnp.sin(own_phase)

    ahead = from_behind(block, "ka", -1)
    ahead_real, ahead_imag = ahead[:, :bands], ahead[:, bands:]
    turned = jnp.concatenate(
        [ahead_real * cosine + ahead_imag * sine, ahead_imag * cosine - ahead_real * sine], axis=1
    )
    weighted = contract(spread, turned, lax.Precision.HIGHEST)
    crossed_weighted = jnp.concatenate([weighted[:, bands:], -weighted[:, :bands]], axis=1)
    result = (
        plane
        + contract(real, weighted, lax.Precision.HIGHEST)
        + contract(imag, crossed_weighted, lax.Precision.HIGHEST)
    )
    summed = scatter_result(result, size, pw_index)
    return summed.reshape(1, bands // size, 2, bands)


def solution(mesh):
    placed = (P("ka", None, "pw", None), P("ka", None, "pw", None), P(), P("pw"), P(), P())
    return jax.shard_map(
        local, mesh=mesh, in_specs=placed, out_specs=P("ka", "pw", None, None), check_vma=False
    )
```

```python
import jax
import jax.numpy as jnp
from jax import lax
from jax.experimental import pallas as pl
from jax.experimental.pallas import tpu as pltpu
from jax.sharding import PartitionSpec as P

PPA = 18


def from_behind(block, axis, distance):
    devices = range(lax.axis_size(axis))
    route = [((i - distance) % len(devices), i) for i in devices]
    return lax.ppermute(block, axis, route)


def contract(left, right, precision=None, kind=jnp.float32):
    return lax.dot_general(
        left,
        right,
        (((0,), (0,)), ((), ())),
        precision=precision,
        preferred_element_type=kind,
    )


def place_kernel(spot_ref, block_ref, out_ref):
    unroll = 16

    def step(i, carry):
        base = pl.multiple_of(i * unroll, unroll)
        rows = [block_ref[pl.ds(base + j, 1), :] for j in range(unroll)]
        for j in range(unroll):
            out_ref[pl.ds(spot_ref[base + j], 1), :] = rows[j]
        return carry

    lax.fori_loop(0, block_ref.shape[0] // unroll, step, 0)


def place_rows(order, block):
    return pl.pallas_call(
        place_kernel,
        out_shape=jax.ShapeDtypeStruct(block.shape, block.dtype),
        in_specs=[
            pl.BlockSpec(memory_space=pltpu.SMEM),
            pl.BlockSpec(memory_space=pltpu.VMEM),
        ],
        out_specs=pl.BlockSpec(memory_space=pltpu.VMEM),
    )(order, block)


def halve(block, names, low):
    at = names.index(low)
    kept = lax.index_in_dim(block, 0, at, keepdims=False)
    sent = lax.index_in_dim(block, 1, at, keepdims=False)
    route = [(i, i ^ low) for i in range(lax.axis_size("pw"))]
    left = [name for name in names if name != low]
    return kept + lax.ppermute(sent, "pw", route), left


def staged(block, names, order):
    for low in order:
        block, names = halve(block, names, low)
    return block


def scatter_result(result, size, pw_index):
    rows = result.shape[0] // size
    if size % 2:
        parts = lax.all_to_all(result.reshape(size, rows, -1), "pw", 0, 0)
        return jnp.sum(parts, axis=0)
    core = pw_index % 2
    split = result.reshape(size // 2, 2, rows, -1)
    kept = lax.dynamic_index_in_dim(split, core, 1, keepdims=False)
    sent = lax.dynamic_index_in_dim(split, 1 - core, 1, keepdims=False)
    joined = kept + lax.ppermute(sent, "pw", [(i, i ^ 1) for i in range(size)])
    groups = [list(range(c, size, 2)) for c in range(2)]
    parts = lax.all_to_all(joined, "pw", 0, 0, axis_index_groups=groups)
    return jnp.sum(parts, axis=0)


def local(waves, projectors, projector_order, shift_map, charges, atom_phase):
    wave = waves[0]
    beta = projectors[0]
    pw_dev, bands = wave.shape[1:]
    size = lax.axis_size("pw")
    last_k = lax.axis_index("ka") == lax.axis_size("ka") - 1
    pw_index = lax.axis_index("pw")
    received = from_behind(wave, "ka", -1)
    straight = jnp.concatenate([wave[0], wave[1]], axis=1)
    crossed = jnp.concatenate([wave[1], -wave[0]], axis=1)
    straight, crossed = lax.optimization_barrier((straight, crossed))
    both = contract(beta[0], straight) + contract(beta[1], crossed)
    rows = beta.shape[2] // size
    if size >= 4 and size & (size - 1) == 0:
        names = [1 << bit for bit in range(size.bit_length() - 1)]
        part = (projector_order // rows) ^ pw_index
        place = jnp.zeros_like(part)
        for low in names:
            place = 2 * place + ((part & low) != 0).astype(jnp.int32)
        spot = place * rows + projector_order % rows
        both = place_rows(spot, both).reshape([2] * len(names) + [rows, 2 * bands])
        real, left = halve(both[..., :bands], names, 1)
        imag, _ = halve(both[..., bands:], names, 1)
        real = staged(real, left, left[1:2] + left[:1] + left[2:])
        imag = staged(imag, left, left)
    else:
        both = lax.psum_scatter(place_rows(projector_order, both), "pw", tiled=True)
        real, imag = both[:, :bands], both[:, bands:]

    spots = lax.iota(jnp.int32, pw_dev)
    local_map = jnp.where(last_k, shift_map - pw_index * pw_dev, spots)
    chosen = (spots[:, None] == local_map[None, :]).astype(jnp.bfloat16)
    joined = jnp.concatenate([received[0], received[1]], axis=1)
    moved = contract(chosen, joined, kind=jnp.bfloat16)
    moved_real, moved_imag = moved[:, :bands], moved[:, bands:]
    plane = contract(wave[0], moved) + contract(
        wave[1], jnp.concatenate([moved_imag, -moved_real], axis=1)
    )

    real, imag, plane = lax.optimization_barrier((real, imag, plane))
    block = jnp.concatenate([real, imag], axis=1)
    atom_dev = block.shape[0] // PPA
    own_charges = lax.dynamic_slice_in_dim(charges, pw_index * atom_dev, atom_dev, 0)
    own_sym = 0.5 * (own_charges + jnp.transpose(own_charges, (0, 2, 1)))
    eye = jnp.eye(atom_dev, dtype=jnp.float32)
    spread = (own_sym[:, :, None, :] * eye[:, None, :, None]).reshape(block.shape[0], block.shape[0])
    own_phase = lax.dynamic_slice_in_dim(atom_phase, pw_index * atom_dev, atom_dev)
    own_phase = jnp.where(last_k, jnp.repeat(own_phase, PPA), 0.0)[:, None]
    cosine, sine = jnp.cos(own_phase), jnp.sin(own_phase)

    ahead = from_behind(block, "ka", -1)
    ahead_real, ahead_imag = ahead[:, :bands], ahead[:, bands:]
    turned = jnp.concatenate(
        [ahead_real * cosine + ahead_imag * sine, ahead_imag * cosine - ahead_real * sine], axis=1
    )
    weighted = contract(spread, turned, lax.Precision.HIGHEST)
    crossed_weighted = jnp.concatenate([weighted[:, bands:], -weighted[:, :bands]], axis=1)
    result = (
        plane
        + contract(real, weighted, lax.Precision.HIGHEST)
        + contract(imag, crossed_weighted, lax.Precision.HIGHEST)
    )
    summed = scatter_result(result, size, pw_index)
    return summed.reshape(1, bands // size, 2, bands)


def solution(mesh):
    placed = (P("ka", None, "pw", None), P("ka", None, "pw", None), P(), P("pw"), P(), P())
    return jax.shard_map(
        local, mesh=mesh, in_specs=placed, out_specs=P("ka", "pw", None, None), check_vma=False
    )
```
